32 devices in a mesh: rows: 2 (over y), hidden: 2 (over x), latents: 8 (over z, core).
Axes of the slice: x: 2, y: 2, z: 4, core: 2. Of those that a mesh axis runs over, the one named last changes fastest.
Arguments:
- inputs: bfloat16 [256, 3584], P('rows', ('hidden', 'latents')), may hold values from -6 to 6
- gate_weight: bfloat16 [3584, 14336], P(None, ('hidden', 'latents')), may hold values from -0.09375 to 0.09375
- up_weight: bfloat16 [3584, 14336], P(None, ('hidden', 'latents')), may hold values from -0.09375 to 0.09375
- down_weight: bfloat16 [14336, 3584], P(('hidden', 'latents')), may hold values from -0.046875 to 0.046875
- encoder: bfloat16 [3584, 65536], P('hidden', ('rows', 'latents')), may hold values from -0.09375 to 0.09375
- decoder: bfloat16 [65536, 3584], P(('rows', 'latents'), 'hidden'), may hold values from -0.09375 to 0.09375
- enc_bias: float32 [65536], P(('rows', 'latents')), may hold values from -3 to 3
- dec_bias: float32 [3584], P('hidden'), may hold values from -3 to 3
- shuffle_order: int32 [256], replicated, may hold values from 0 to 255, each once
Outputs:
- recon_out: bfloat16 [256, 3584], P(('rows', 'latents'), 'hidden')
- grad_enc: bfloat16 [3584, 65536], P('hidden', ('rows', 'latents'))
- grad_dec: bfloat16 [65536, 3584], P(('rows', 'latents'), 'hidden')
The draws below stay inside these ranges and needn't reach their ends.
Inputs may be any that keep to these rules, and one draw needn't show every extreme that they name: shuffle_order names every token index 0 to 255 exactly once.
All inputs are finite; a program needn't handle non-finite values.
Results may differ from the reference program's by a relative error of at most 0.038.
Values may be sent and summed in bfloat16 or wider, within the bound.
A program may use at most 128 MiB of HBM per device.

```python
import math
import jax
import jax.numpy as jnp
from jax import lax

D = 3584
FF = 14336
LATENTS = 65536
TOKENS = 256
N_HIDDEN = 2


def steps_of(stream_key, dims, cuts, least, largest):
    loudness, own = 1.0, jax.random.fold_in(stream_key, 6)
    for position, shards_of in cuts:
        heights = jnp.exp(jax.random.uniform(jax.random.fold_in(own, position), (shards_of,), jnp.float32, least / len(cuts), largest / len(cuts)))
        loudness = loudness * jnp.repeat(heights, dims[position] // shards_of).reshape([-1 if axis == position else 1 for axis in range(len(dims))])
    return loudness


def gaussian(rng, shape, scale, bound, cuts=(), dtype=jnp.bfloat16):
    gain = steps_of(rng, shape, cuts, -0.22, 0.18) if cuts else 1.0
    result = jax.random.normal(rng, shape, jnp.float32) * scale * gain
    return jnp.minimum(jnp.maximum(result, -bound), bound).astype(dtype)


def setup_inputs(seed: int = 0) -> dict:
    key_list = jax.random.split(jax.random.key(seed), 10)
    return {
        "inputs": gaussian(key_list[0], (TOKENS, D), 1.0, 6.0, ((0, 2), (1, 16))),
        "gate_weight": gaussian(key_list[1], (D, FF), D ** -0.5, 0.09375, ((1, 16),)),
        "up_weight": gaussian(key_list[2], (D, FF), D ** -0.5, 0.09375, ((1, 16),)),
        "down_weight": gaussian(key_list[3], (FF, D), FF ** -0.5, 0.046875, ((0, 16),)),
        "encoder": gaussian(key_list[4], (D, LATENTS), D ** -0.5, 0.09375, ((0, 2), (1, 16))),
        "decoder": gaussian(key_list[5], (LATENTS, D), D ** -0.5, 0.09375, ((0, 16), (1, 2))),
        "enc_bias": gaussian(key_list[6], (LATENTS,), 0.5, 3.0, ((0, 16),), jnp.float32),
        "dec_bias": gaussian(key_list[7], (D,), 0.5, 3.0, ((0, 2),), jnp.float32),
        "shuffle_order": jax.random.permutation(key_list[8], TOKENS).astype(jnp.int32),
    }


smooth_scale = 0.1
sparsity_weight = 0.5

def blockwise(left, right_rows):
    width = D // N_HIDDEN
    total = None
    for shard in range(N_HIDDEN):
        piece = jnp.dot(left[:, shard * width:(shard + 1) * width], right_rows[shard * width:(shard + 1) * width, :], preferred_element_type=jnp.float32)
        piece = lax.optimization_barrier(piece.astype(jnp.bfloat16)).astype(jnp.float32)
        total = piece if total is None else total + piece
    return total

def reference(inputs, gate_weight, up_weight, down_weight, encoder, decoder, enc_bias, dec_bias, shuffle_order):
    gate_act = jnp.dot(inputs, gate_weight, preferred_element_type=jnp.float32)
    up_act = jnp.dot(inputs, up_weight, preferred_element_type=jnp.float32)
    hidden = (jax.nn.gelu(gate_act, approximate=True) * up_act).astype(jnp.bfloat16)
    mlp_out = jnp.dot(hidden, down_weight, preferred_element_type=jnp.float32).astype(jnp.bfloat16)
    shuffled = jnp.take(mlp_out, shuffle_order.astype(jnp.int32), axis=0)
    pre_act = blockwise(shuffled, encoder) + enc_bias[None, :]
    latent_act = (smooth_scale * jax.nn.softplus(pre_act / smooth_scale)).astype(jnp.bfloat16)
    recon = jnp.dot(latent_act, decoder, preferred_element_type=jnp.float32) + dec_bias[None, :]
    recon_out = recon.astype(jnp.bfloat16)
    scale = 1.0 / math.sqrt(TOKENS)
    d_err = (scale * (recon - shuffled.astype(jnp.float32))).astype(jnp.bfloat16)
    grad_dec = jnp.dot(latent_act.T, d_err, preferred_element_type=jnp.float32).astype(jnp.bfloat16)
    d_latent = blockwise(d_err, decoder.T)
    d_pre = ((d_latent + sparsity_weight * scale) * jax.nn.sigmoid(pre_act / smooth_scale)).astype(jnp.bfloat16)
    grad_enc = jnp.dot(shuffled.T, d_pre, preferred_element_type=jnp.float32).astype(jnp.bfloat16)
    return (recon_out, grad_enc, grad_dec)
```

```python
import functools
import math

import jax
import jax.numpy as jnp
from jax import lax
from jax.experimental import pallas as pl
from jax.experimental.pallas import tpu as pltpu
from jax.sharding import PartitionSpec as P

smooth_scale = 0.1
sparsity_weight = 0.5
chunks = 4
MESH = pl.DeviceIdType.MESH


class Places:
    def __init__(self, depths):
        here = lax.axis_index("latents")
        self.depths = depths
        self.core = lax.rem(here, 2)
        self.depth = lax.div(here, 2)
        self.latents = here

    def ahead(self, step):
        return lax.rem(self.depth + step, self.depths)

    def behind(self, step):
        return lax.rem(self.depth + self.depths - step, self.depths)

    def to_core(self):
        return {"latents": self.depth * 2 + 1 - self.core}

    def to_depth(self, depth):
        return {"latents": depth * 2 + self.core}


def to_pair(axis):
    return {axis: 1 - lax.axis_index(axis)}


def greet(places, axes):
    barrier = pltpu.get_barrier_semaphore()
    targets = [places.to_core()] + [to_pair(axis) for axis in axes]
    targets += [places.to_depth(places.ahead(step)) for step in range(1, places.depths)]
    for target in targets:
        pl.semaphore_signal(barrier, inc=1, device_id=target, device_id_type=MESH)
    pl.semaphore_wait(barrier, len(targets))


def send(source, target, sems, number, device):
    copy = pltpu.make_async_remote_copy(
        src_ref=source,
        dst_ref=target,
        send_sem=sems.at[0, number],
        recv_sem=sems.at[1, number],
        device_id=device,
        device_id_type=MESH,
    )
    copy.start()
    return copy


def spread(places, axis, pieces, sems):
    pair, core, depths = lax.axis_index(axis), places.core, places.depths
    own = pieces.at[pair, places.depth, core]
    along, across, inside = [], [], []
    for step in range(1, depths):
        along.append(
            send(own, own, sems, step - 1, places.to_depth(places.ahead(step)))
        )
    across.append(send(own, own, sems, depths, to_pair(axis)))
    inside.append(send(own, own, sems, 2 * depths, places.to_core()))
    for step in range(1, depths):
        along[step - 1].wait_recv()
        piece = pieces.at[pair, places.behind(step), core]
        across.append(send(piece, piece, sems, depths + step, to_pair(axis)))
        inside.append(send(piece, piece, sems, 2 * depths + step, places.to_core()))
    for step in range(depths):
        across[step].wait_recv()
        piece = pieces.at[1 - pair, places.behind(step), core]
        inside.append(
            send(piece, piece, sems, 3 * depths + step, places.to_core())
        )
    for copy in inside:
        copy.wait_recv()
    for copy in along + across + inside:
        copy.wait_send()


def gather_kernel(axis, depths, x_ref, out_ref, pieces, sems):
    places = Places(depths)
    greet(places, (axis,))
    pieces[lax.axis_index(axis), places.depth, places.core] = x_ref[...]
    spread(places, axis, pieces, sems)
    out_ref[...] = pieces[...]


def exchange_sum(places, axis, mine, other, theirs, from_pair, to_send, from_depth, sems):
    depths = places.depths
    order = list(range(1, depths)) + [0]
    across = []
    for step in order:
        depth = places.ahead(step)
        theirs[depth] = other(depth).astype(theirs.dtype)
        across.append(
            send(theirs.at[depth], from_pair.at[depth], sems, step, to_pair(axis))
        )
    along = []
    for place, step in enumerate(order):
        depth = places.ahead(step)
        across[place].wait_recv()
        total = mine(depth) + from_pair[depth].astype(jnp.float32)
        if step:
            to_send[step - 1] = total.astype(to_send.dtype)
            along.append(
                send(
                    to_send.at[step - 1],
                    from_depth.at[step - 1],
                    sems,
                    depths + step,
                    places.to_depth(depth),
                )
            )
    for step in range(1, depths):
        along[step - 1].wait_recv()
        total = total + from_depth[step - 1].astype(jnp.float32)
    for copy in across + along:
        copy.wait_send()
    return total


def rows_kernel(
    depths, x_ref, out_ref, from_core, theirs, from_pair, to_send, from_depth, pieces, sems, more
):
    places = Places(depths)
    core, side = places.core, lax.axis_index("hidden")
    width = out_ref.shape[-1]
    greet(places, ("hidden", "rows"))
    halves = send(x_ref.at[:, 1 - core], from_core, sems, 2 * depths, places.to_core())
    halves.wait_recv()

    def part(which):
        columns = pl.ds(pl.multiple_of(which * width, 128), width)

        def at(depth):
            own = x_ref[depth, core, :, columns].astype(jnp.float32)
            return own + from_core[depth, :, columns].astype(jnp.float32)

        return at

    total = exchange_sum(
        places, "hidden", part(side), part(1 - side), theirs, from_pair, to_send, from_depth, sems
    )
    pieces[lax.axis_index("rows"), places.depth, core] = total.astype(pieces.dtype)
    halves.wait_send()
    spread(places, "rows", pieces, more)
    out_ref[...] = pieces[...]


def recon_kernel(
    depths,
    scale,
    x_ref,
    target_ref,
    bias_ref,
    err_ref,
    recon_ref,
    from_core,
    theirs,
    from_pair,
    to_send,
    from_depth,
    pieces,
    sems,
    more,
):
    places = Places(depths)
    core, side = places.core, lax.axis_index("rows")
    greet(places, ("rows",))
    halves = send(x_ref.at[:, :, 1 - core], from_core, sems, 2 * depths, places.to_core())
    halves.wait_recv()

    def part(which):
        def at(depth):
            own = x_ref[which, depth, core].astype(jnp.float32)
            return own + from_core[which, depth].astype(jnp.float32)

        return at

    total = exchange_sum(
        places, "rows", part(side), part(1 - side), theirs, from_pair, to_send, from_depth, sems
    )
    recon = total + bias_ref[...]
    recon_ref[...] = recon.astype(recon_ref.dtype)
    err = scale * (recon - target_ref[side, places.depth, core].astype(jnp.float32))
    pieces[side, places.depth, core] = err.astype(pieces.dtype)
    halves.wait_send()
    spread(places, "rows", pieces, more)
    err_ref[...] = pieces[...]


def vmem(count):
    return [pl.BlockSpec(memory_space=pltpu.VMEM)] * count


def params(number):
    return pltpu.CompilerParams(collective_id=number, has_side_effects=True)


def gather_features(x, depths):
    shape = (2, depths, 2) + x.shape
    out = pl.pallas_call(
        functools.partial(gather_kernel, "hidden", depths),
        out_shape=jax.ShapeDtypeStruct(shape, x.dtype),
        in_specs=vmem(1),
        out_specs=vmem(1)[0],
        scratch_shapes=[
            pltpu.VMEM(shape, x.dtype),
            pltpu.SemaphoreType.DMA((2, 4 * depths)),
        ],
        compiler_params=params(0),
        name="gather_features",
    )(x)
    return out.reshape(-1, x.shape[-1])


def reduce_scratch(depths, rows, width, core_shape, dtype):
    piece = (rows, width)
    return [
        pltpu.VMEM(core_shape, dtype),
        pltpu.VMEM((depths,) + piece, dtype),
        pltpu.VMEM((depths,) + piece, dtype),
        pltpu.VMEM((depths - 1,) + piece, dtype),
        pltpu.VMEM((depths - 1,) + piece, dtype),
        pltpu.VMEM((2, depths, 2) + piece, dtype),
        pltpu.SemaphoreType.DMA((2, 2 * depths + 1)),
        pltpu.SemaphoreType.DMA((2, 4 * depths)),
    ]


def sum_rows(x, depths):
    rows, width = x.shape[0] // (2 * depths), x.shape[1] // 2
    out = pl.pallas_call(
        functools.partial(rows_kernel, depths),
        out_shape=jax.ShapeDtypeStruct((2, depths, 2, rows, width), x.dtype),
        in_specs=vmem(1),
        out_specs=vmem(1)[0],
        scratch_shapes=reduce_scratch(
            depths, rows, width, (depths, rows, x.shape[1]), x.dtype
        ),
        compiler_params=params(1),
        name="sum_rows",
    )(x.reshape(depths, 2, rows, x.shape[1]))
    return out.reshape(-1, width)


def sum_recon(x, target, bias, scale, depths):
    tokens, width = x.shape
    rows = tokens // (4 * depths)
    shape = (2, depths, 2, rows, width)
    err, recon = pl.pallas_call(
        functools.partial(recon_kernel, depths, scale),
        out_shape=(
            jax.ShapeDtypeStruct(shape, x.dtype),
            jax.ShapeDtypeStruct((rows, width), x.dtype),
        ),
        in_specs=vmem(3),
        out_specs=tuple(vmem(2)),
        scratch_shapes=reduce_scratch(depths, rows, width, (2, depths, rows, width), x.dtype),
        compiler_params=params(2),
        name="sum_recon",
    )(x.reshape(shape), target.reshape(shape), bias[None, :])
    return err.reshape(tokens, width), recon


def add_pair(x):
    if lax.axis_size("hidden") == 2:
        other = lax.ppermute(x, "hidden", [(0, 1), (1, 0)])
        return x.astype(jnp.float32) + other.astype(jnp.float32)
    return lax.psum(x, "hidden").astype(jnp.float32)


def shards(
    inputs, gate_weight, up_weight, down_weight, encoder, decoder, enc_bias, dec_bias, shuffle_order
):
    rows_n, hidden_n, latents_n = map(lax.axis_size, ("rows", "hidden", "latents"))
    tokens = shuffle_order.shape[0]
    features = gate_weight.shape[0]
    depths = latents_n // 2
    fast = (
        rows_n == 2
        and hidden_n == 2
        and latents_n % 2 == 0
        and tokens % (2 * latents_n * 16) == 0
        and features % 256 == 0
        and inputs.shape[1] % 16 == 0
        and inputs.shape[0] % 128 == 0
    )
    if fast:
        gathered = gather_features(inputs.T, depths).T
    else:
        gathered = lax.all_gather(inputs, ("hidden", "latents"), axis=1, tiled=True)
    gate_act = jnp.dot(gathered, gate_weight, preferred_element_type=jnp.float32)
    up_act = jnp.dot(gathered, up_weight, preferred_element_type=jnp.float32)
    hidden = (jax.nn.gelu(gate_act, approximate=True) * up_act).astype(jnp.bfloat16)
    partial_value = jnp.dot(hidden, down_weight, preferred_element_type=jnp.float32)
    partial_value = partial_value.astype(jnp.bfloat16)
    if fast:
        every_row = sum_rows(partial_value, depths)
    else:
        share = lax.psum_scatter(partial_value, "hidden", scatter_dimension=1, tiled=True)
        width_rows = lax.psum(share, "latents")
        every_row = lax.all_gather(width_rows, "rows", axis=0, tiled=True)
    shuffled = jnp.take(every_row, shuffle_order, axis=0)

    count = chunks if encoder.shape[1] % (128 * chunks) == 0 else 1
    size = encoder.shape[1] // count
    cuts = [slice(i * size, (i + 1) * size) for i in range(count)]
    pre_act, latent_act = [], []
    recon_local = None
    for cut in cuts:
        pre_local = jnp.dot(shuffled, encoder[:, cut], preferred_element_type=jnp.float32)
        pre = add_pair(pre_local.astype(jnp.bfloat16)) + enc_bias[None, cut]
        pre_act.append(pre)
        latent = (smooth_scale * jax.nn.softplus(pre / smooth_scale)).astype(jnp.bfloat16)
        latent_act.append(latent)
        term = jnp.dot(latent, decoder[cut], preferred_element_type=jnp.float32)
        recon_local = term if recon_local is None else recon_local + term
    scale = 1.0 / math.sqrt(tokens)
    if fast:
        d_err, recon_out = sum_recon(
            recon_local.astype(jnp.bfloat16), shuffled, dec_bias, scale, depths
        )
    else:
        recon = lax.psum(recon_local, ("rows", "latents")) + dec_bias[None, :]
        recon_full = recon.astype(jnp.bfloat16)
        d_err = (scale * (recon - shuffled.astype(jnp.float32))).astype(jnp.bfloat16)
        row_count = tokens // (rows_n * latents_n)
        first_row = lax.axis_index(("rows", "latents")) * row_count
        recon_out = lax.dynamic_slice_in_dim(recon_full, first_row, row_count, 0)
    d_pre = []
    for cut, pre in zip(cuts, pre_act):
        back_local = lax.dot_general(
            d_err, decoder[cut], (((1,), (1,)), ((), ())), preferred_element_type=jnp.float32
        )
        d_latent = add_pair(back_local.astype(jnp.bfloat16))
        d_pre.append(
            (
                (d_latent + sparsity_weight * scale) * jax.nn.sigmoid(pre / smooth_scale)
            ).astype(jnp.bfloat16)
        )
    grad_dec = lax.dot_general(
        jnp.concatenate(latent_act, axis=1),
        d_err,
        (((0,), (0,)), ((), ())),
        preferred_element_type=jnp.float32,
    ).astype(jnp.bfloat16)
    grad_enc = lax.dot_general(
        shuffled,
        jnp.concatenate(d_pre, axis=1),
        (((0,), (0,)), ((), ())),
        preferred_element_type=jnp.float32,
    ).astype(jnp.bfloat16)
    return (recon_out, grad_enc, grad_dec)


def solution(mesh):
    return jax.shard_map(
        shards,
        mesh=mesh,
        in_specs=(
            P("rows", ("hidden", "latents")),
            P(None, ("hidden", "latents")),
            P(None, ("hidden", "latents")),
            P(("hidden", "latents"), None),
            P("hidden", ("rows", "latents")),
            P(("rows", "latents"), "hidden"),
            P(("rows", "latents")),
            P("hidden"),
            P(),
        ),
        out_specs=(
            P(("rows", "latents"), "hidden"),
            P("hidden", ("rows", "latents")),
            P(("rows", "latents"), "hidden"),
        ),
        check_vma=False,
    )
```

```python
import functools
import math

import jax
import jax.numpy as jnp
from jax import lax
from jax.experimental import pallas as pl
from jax.experimental.pallas import tpu as pltpu
from jax.sharding import PartitionSpec as P


smooth_scale = 0.1
sparsity_weight = 0.5
chunks = 2
halves = 2
MESH = pl.DeviceIdType.MESH


class Places:
    def __init__(self, depths):
        here = lax.axis_index("latents")
        self.depths = depths
        self.core = lax.rem(here, 2)
        self.depth = lax.div(here, 2)

    def ahead(self, step):
        return lax.rem(self.depth + step, self.depths)

    def behind(self, step):
        return lax.rem(self.depth + self.depths - step, self.depths)

    def to_core(self):
        return {"latents": self.depth * 2 + 1 - self.core}

    def to_depth(self, depth):
        return {"latents": depth * 2 + self.core}


def to_pair(axis):
    return {axis: 1 - lax.axis_index(axis)}


def greet(places, axes):
    barrier = pltpu.get_barrier_semaphore()
    targets = [places.to_core()] + [to_pair(axis) for axis in axes]
    targets += [places.to_depth(places.ahead(step)) for step in range(1, places.depths)]
    for target in targets:
        pl.semaphore_signal(barrier, inc=1, device_id=target, device_id_type=MESH)
    pl.semaphore_wait(barrier, len(targets))


def send(source, target, sems, number, device):
    copy = pltpu.make_async_remote_copy(
        src_ref=source,
        dst_ref=target,
        send_sem=sems.at[0, number],
        recv_sem=sems.at[1, number],
        device_id=device,
        device_id_type=MESH,
    )
    copy.start()
    return copy


def spread(places, axis, pieces, sems):
    pair, core, depths = lax.axis_index(axis), places.core, places.depths
    own = pieces.at[pair, places.depth, core]
    along, across, inside = [], [], []
    for step in range(1, depths):
        along.append(
            send(own, own, sems, step - 1, places.to_depth(places.ahead(step)))
        )
    across.append(send(own, own, sems, depths, to_pair(axis)))
    inside.append(send(own, own, sems, 2 * depths, places.to_core()))
    for step in range(1, depths):
        along[step - 1].wait_recv()
        piece = pieces.at[pair, places.behind(step), core]
        across.append(send(piece, piece, sems, depths + step, to_pair(axis)))
        inside.append(send(piece, piece, sems, 2 * depths + step, places.to_core()))
    for step in range(depths):
        across[step].wait_recv()
        piece = pieces.at[1 - pair, places.behind(step), core]
        inside.append(
            send(piece, piece, sems, 3 * depths + step, places.to_core())
        )
    for copy in inside:
        copy.wait_recv()
    for copy in along + across + inside:
        copy.wait_send()


def gather_kernel(axis, depths, x_ref, out_ref, pieces, sems):
    places = Places(depths)
    greet(places, (axis,))
    pieces[lax.axis_index(axis), places.depth, places.core] = x_ref[...]
    spread(places, axis, pieces, sems)
    out_ref[...] = pieces[...]


def exchange_sum(places, axis, mine, other, theirs, from_pair, to_send, from_depth, sems):
    depths = places.depths
    order = list(range(1, depths)) + [0]
    across = []
    for step in order:
        depth = places.ahead(step)
        theirs[depth] = other(depth).astype(theirs.dtype)
        across.append(
            send(theirs.at[depth], from_pair.at[depth], sems, step, to_pair(axis))
        )
    along = []
    for place, step in enumerate(order):
        depth = places.ahead(step)
        across[place].wait_recv()
        total = mine(depth) + from_pair[depth].astype(jnp.float32)
        if step:
            to_send[step - 1] = total.astype(to_send.dtype)
            along.append(
                send(
                    to_send.at[step - 1],
                    from_depth.at[step - 1],
                    sems,
                    depths + step,
                    places.to_depth(depth),
                )
            )
    for step in range(1, depths):
        along[step - 1].wait_recv()
        total = total + from_depth[step - 1].astype(jnp.float32)
    for copy in across + along:
        copy.wait_send()
    return total


def rows_kernel(
    depths, x_ref, out_ref, from_core, theirs, from_pair, to_send, from_depth, pieces, sems, more
):
    places = Places(depths)
    core, side = places.core, lax.axis_index("hidden")
    width = out_ref.shape[-1]
    greet(places, ("hidden", "rows"))
    halves = send(x_ref.at[:, 1 - core], from_core, sems, 2 * depths, places.to_core())
    halves.wait_recv()

    def part(which):
        columns = pl.ds(pl.multiple_of(which * width, 128), width)

        def at(depth):
            own = x_ref[depth, core, :, columns].astype(jnp.float32)
            return own + from_core[depth, :, columns].astype(jnp.float32)

        return at

    total = exchange_sum(
        places, "hidden", part(side), part(1 - side), theirs, from_pair, to_send, from_depth, sems
    )
    pieces[lax.axis_index("rows"), places.depth, core] = total.astype(pieces.dtype)
    halves.wait_send()
    spread(places, "rows", pieces, more)
    out_ref[...] = pieces[...]


def recon_kernel(
    depths,
    scale,
    x_ref,
    target_ref,
    bias_ref,
    err_ref,
    recon_ref,
    from_core,
    theirs,
    from_pair,
    to_send,
    from_depth,
    pieces,
    sems,
    more,
):
    places = Places(depths)
    core, side = places.core, lax.axis_index("rows")
    greet(places, ("rows",))
    halves = send(x_ref.at[:, :, 1 - core], from_core, sems, 2 * depths, places.to_core())
    halves.wait_recv()

    def part(which):
        def at(depth):
            own = x_ref[which, depth, core].astype(jnp.float32)
            return own + from_core[which, depth].astype(jnp.float32)

        return at

    total = exchange_sum(
        places, "rows", part(side), part(1 - side), theirs, from_pair, to_send, from_depth, sems
    )
    recon = total + bias_ref[...]
    recon_ref[...] = recon.astype(recon_ref.dtype)
    err = scale * (recon - target_ref[side, places.depth, core].astype(jnp.float32))
    pieces[side, places.depth, core] = err.astype(pieces.dtype)
    halves.wait_send()
    spread(places, "rows", pieces, more)
    err_ref[...] = pieces[...]


def vmem(count):
    return [pl.BlockSpec(memory_space=pltpu.VMEM)] * count


def params(number):
    return pltpu.CompilerParams(collective_id=number, has_side_effects=True)


def gather_features(x, depths):
    shape = (2, depths, 2) + x.shape
    out = pl.pallas_call(
        functools.partial(gather_kernel, "hidden", depths),
        out_shape=jax.ShapeDtypeStruct(shape, x.dtype),
        in_specs=vmem(1),
        out_specs=vmem(1)[0],
        scratch_shapes=[
            pltpu.VMEM(shape, x.dtype),
            pltpu.SemaphoreType.DMA((2, 4 * depths)),
        ],
        compiler_params=params(0),
        name="gather_features",
    )(x)
    return out.reshape(-1, x.shape[-1])


def reduce_scratch(depths, rows, width, core_shape, dtype):
    piece = (rows, width)
    return [
        pltpu.VMEM(core_shape, dtype),
        pltpu.VMEM((depths,) + piece, dtype),
        pltpu.VMEM((depths,) + piece, dtype),
        pltpu.VMEM((depths - 1,) + piece, dtype),
        pltpu.VMEM((depths - 1,) + piece, dtype),
        pltpu.VMEM((2, depths, 2) + piece, dtype),
        pltpu.SemaphoreType.DMA((2, 2 * depths + 1)),
        pltpu.SemaphoreType.DMA((2, 4 * depths)),
    ]


def sum_rows(x, depths):
    rows, width = x.shape[0] // (2 * depths), x.shape[1] // 2
    out = pl.pallas_call(
        functools.partial(rows_kernel, depths),
        out_shape=jax.ShapeDtypeStruct((2, depths, 2, rows, width), x.dtype),
        in_specs=vmem(1),
        out_specs=vmem(1)[0],
        scratch_shapes=reduce_scratch(
            depths, rows, width, (depths, rows, x.shape[1]), x.dtype
        ),
        compiler_params=params(1),
        name="sum_rows",
    )(x.reshape(depths, 2, rows, x.shape[1]))
    return out.reshape(-1, width)


def sum_recon(x, target, bias, scale, depths, number):
    tokens, width = x.shape
    rows = tokens // (4 * depths)
    shape = (2, depths, 2, rows, width)
    err, recon = pl.pallas_call(
        functools.partial(recon_kernel, depths, scale),
        out_shape=(
            jax.ShapeDtypeStruct(shape, x.dtype),
            jax.ShapeDtypeStruct((rows, width), x.dtype),
        ),
        in_specs=vmem(3),
        out_specs=tuple(vmem(2)),
        scratch_shapes=reduce_scratch(depths, rows, width, (2, depths, rows, width), x.dtype),
        compiler_params=params(number),
    )(x.reshape(shape), target.reshape(shape), bias[None, :])
    return err.reshape(tokens, width), recon


def after(x, *others):
    return lax.optimization_barrier((x,) + others)[0]


def add_pair(x, *others):
    if lax.axis_size("hidden") == 2:
        other = lax.ppermute(x, "hidden", [(0, 1), (1, 0)])
        other = after(other, *others) if others else other
        return x.astype(jnp.float32) + other.astype(jnp.float32)
    return lax.psum(x, "hidden").astype(jnp.float32)


def shards(
    inputs, gate_weight, up_weight, down_weight, encoder, decoder, enc_bias, dec_bias, shuffle_order
):
    rows_n, hidden_n, latents_n = map(lax.axis_size, ("rows", "hidden", "latents"))
    tokens = shuffle_order.shape[0]
    features = gate_weight.shape[0]
    depths = latents_n // 2
    fast = (
        rows_n == 2
        and hidden_n == 2
        and latents_n % 2 == 0
        and tokens % (2 * latents_n * 16) == 0
        and features % 256 == 0
        and inputs.shape[1] % 16 == 0
        and inputs.shape[0] % 128 == 0
    )
    if fast:
        gathered = gather_features(inputs.T, depths).T
    else:
        gathered = lax.all_gather(inputs, ("hidden", "latents"), axis=1, tiled=True)
    gate_act = jnp.dot(gathered, gate_weight, preferred_element_type=jnp.float32)
    up_act = jnp.dot(gathered, up_weight, preferred_element_type=jnp.float32)
    hidden = (jax.nn.gelu(gate_act, approximate=True) * up_act).astype(jnp.bfloat16)
    partial_value = jnp.dot(hidden, down_weight, preferred_element_type=jnp.float32)
    partial_value = partial_value.astype(jnp.bfloat16)
    if fast:
        every_row = sum_rows(partial_value, depths)
    else:
        share = lax.psum_scatter(partial_value, "hidden", scatter_dimension=1, tiled=True)
        width_rows = lax.psum(share, "latents")
        every_row = lax.all_gather(width_rows, "rows", axis=0, tiled=True)
    scale = 1.0 / math.sqrt(tokens)
    order = shuffle_order
    if fast:
        order = order.reshape(rows_n * latents_n, halves, -1).transpose(1, 0, 2).reshape(-1)
    columns = lax.broadcasted_iota(jnp.int32, (tokens, tokens), 1)
    one_hot = (order[:, None] == columns).astype(jnp.bfloat16)
    shuffled = jnp.dot(one_hot, every_row, preferred_element_type=jnp.float32)
    shuffled = shuffled.astype(jnp.bfloat16)

    count = chunks if encoder.shape[1] % (128 * chunks) == 0 else 1
    size = encoder.shape[1] // count
    cuts = [slice(i * size, (i + 1) * size) for i in range(count)]
    parts = halves if fast else 1
    share = tokens // parts
    rows = [shuffled[i * share : (i + 1) * share] for i in range(parts)]
    local = []
    for part in range(parts):
        if part:
            rows[part] = after(rows[part], *local[part - 1])
        local.append(
            [
                jnp.dot(
                    rows[part], encoder[:, cut], preferred_element_type=jnp.float32
                ).astype(jnp.bfloat16)
                for cut in cuts
            ]
        )
    pre_act, latent_act, recon_out, d_err, d_pre = [], [], [], [], []
    for part in range(parts):
        pre, latent = [], []
        recon_local = None
        for i, cut in enumerate(cuts):
            summed = add_pair(local[part][i], *d_err[part - 1 : part])
            pre.append(summed + enc_bias[None, cut])
            latent.append(
                (smooth_scale * jax.nn.softplus(pre[i] / smooth_scale)).astype(jnp.bfloat16)
            )
            term = jnp.dot(latent[i], decoder[cut], preferred_element_type=jnp.float32)
            recon_local = term if recon_local is None else recon_local + term
        pre_act.append(pre)
        latent_act.append(jnp.concatenate(latent, axis=1))
        if fast:
            err, recon_rows = sum_recon(
                recon_local.astype(jnp.bfloat16), rows[part], dec_bias, scale, depths, 2 + part
            )
        else:
            recon = lax.psum(recon_local, ("rows", "latents")) + dec_bias[None, :]
            err = (scale * (recon - rows[part].astype(jnp.float32))).astype(jnp.bfloat16)
            row_count = tokens // (rows_n * latents_n)
            first_row = lax.axis_index(("rows", "latents")) * row_count
            recon_rows = lax.dynamic_slice_in_dim(
                recon.astype(jnp.bfloat16), first_row, row_count, 0
            )
        recon_out.append(recon_rows)
        d_err.append(err)
    for part in range(parts):
        d_pre.append([])
        for i, cut in enumerate(cuts):
            back_local = lax.dot_general(
                d_err[part],
                decoder[cut],
                (((1,), (1,)), ((), ())),
                preferred_element_type=jnp.float32,
            ).astype(jnp.bfloat16)
            d_latent = add_pair(back_local)
            gate = jax.nn.sigmoid(pre_act[part][i] / smooth_scale)
            d_pre[part].append(
                ((d_latent + sparsity_weight * scale) * gate).astype(jnp.bfloat16)
            )
    grad_dec = lax.dot_general(
        jnp.concatenate(latent_act, axis=0),
        jnp.concatenate(d_err, axis=0),
        (((0,), (0,)), ((), ())),
        preferred_element_type=jnp.float32,
    ).astype(jnp.bfloat16)
    grad_enc = lax.dot_general(
        shuffled,
        jnp.concatenate([jnp.concatenate(part, axis=1) for part in d_pre], axis=0),
        (((0,), (0,)), ((), ())),
        preferred_element_type=jnp.float32,
    ).astype(jnp.bfloat16)
    return (jnp.concatenate(recon_out, axis=0), grad_enc, grad_dec)


def solution(mesh):
    return jax.shard_map(
        shards,
        mesh=mesh,
        in_specs=(
            P("rows", ("hidden", "latents")),
            P(None, ("hidden", "latents")),
            P(None, ("hidden", "latents")),
            P(("hidden", "latents"), None),
            P("hidden", ("rows", "latents")),
            P(("rows", "latents"), "hidden"),
            P(("rows", "latents")),
            P("hidden"),
            P(),
        ),
        out_specs=(
            P(("rows", "latents"), "hidden"),
            P("hidden", ("rows", "latents")),
            P(("rows", "latents"), "hidden"),
        ),
        check_vma=False,
    )
```

```python
import functools
import math

import jax
import jax.numpy as jnp
from jax import lax
from jax.experimental import pallas as pl
from jax.experimental.pallas import tpu as pltpu
from jax.sharding import PartitionSpec as P


smooth_scale = 0.1
sparsity_weight = 0.5
chunks = 2
halves = 2
turn_kernels = True
MESH = pl.DeviceIdType.MESH


class Places:
    def __init__(self, depths):
        here = lax.axis_index("latents")
        self.depths = depths
        self.core = lax.rem(here, 2)
        self.depth = lax.div(here, 2)

    def ahead(self, step):
        return lax.rem(self.depth + step, self.depths)

    def behind(self, step):
        return lax.rem(self.depth + self.depths - step, self.depths)

    def to_core(self):
        return {"latents": self.depth * 2 + 1 - self.core}

    def to_depth(self, depth):
        return {"latents": depth * 2 + self.core}


def to_pair(axis):
    return {axis: 1 - lax.axis_index(axis)}


def greet(places, axes):
    barrier = pltpu.get_barrier_semaphore()
    targets = [places.to_core()] + [to_pair(axis) for axis in axes]
    targets += [places.to_depth(places.ahead(step)) for step in range(1, places.depths)]
    for target in targets:
        pl.semaphore_signal(barrier, inc=1, device_id=target, device_id_type=MESH)
    pl.semaphore_wait(barrier, len(targets))


def send(source, target, sems, number, device):
    copy = pltpu.make_async_remote_copy(
        src_ref=source,
        dst_ref=target,
        send_sem=sems.at[0, number],
        recv_sem=sems.at[1, number],
        device_id=device,
        device_id_type=MESH,
    )
    copy.start()
    return copy


def spread(places, axis, pieces, sems):
    pair, core, depths = lax.axis_index(axis), places.core, places.depths
    own = pieces.at[pair, places.depth, core]
    along, across, inside = [], [], []
    for step in range(1, depths):
        along.append(
            send(own, own, sems, step - 1, places.to_depth(places.ahead(step)))
        )
    across.append(send(own, own, sems, depths, to_pair(axis)))
    inside.append(send(own, own, sems, 2 * depths, places.to_core()))
    for step in range(1, depths):
        along[step - 1].wait_recv()
        piece = pieces.at[pair, places.behind(step), core]
        across.append(send(piece, piece, sems, depths + step, to_pair(axis)))
        inside.append(send(piece, piece, sems, 2 * depths + step, places.to_core()))
    for step in range(depths):
        across[step].wait_recv()
        piece = pieces.at[1 - pair, places.behind(step), core]
        inside.append(
            send(piece, piece, sems, 3 * depths + step, places.to_core())
        )
    for copy in inside:
        copy.wait_recv()
    for copy in along + across + inside:
        copy.wait_send()


def gather_kernel(axis, depths, x_ref, out_ref, pieces, sems):
    places = Places(depths)
    greet(places, (axis,))
    pieces[lax.axis_index(axis), places.depth, places.core] = x_ref[...]
    spread(places, axis, pieces, sems)
    out_ref[...] = pieces[...]


def exchange_sum(places, axis, mine, other, theirs, from_pair, to_send, from_depth, sems):
    depths = places.depths
    order = list(range(1, depths)) + [0]
    across = []
    for step in order:
        depth = places.ahead(step)
        theirs[depth] = other(depth).astype(theirs.dtype)
        across.append(
            send(theirs.at[depth], from_pair.at[depth], sems, step, to_pair(axis))
        )
    along = []
    for place, step in enumerate(order):
        depth = places.ahead(step)
        across[place].wait_recv()
        total = mine(depth) + from_pair[depth].astype(jnp.float32)
        if step:
            to_send[step - 1] = total.astype(to_send.dtype)
            along.append(
                send(
                    to_send.at[step - 1],
                    from_depth.at[step - 1],
                    sems,
                    depths + step,
                    places.to_depth(depth),
                )
            )
    for step in range(1, depths):
        along[step - 1].wait_recv()
        total = total + from_depth[step - 1].astype(jnp.float32)
    for copy in across + along:
        copy.wait_send()
    return total


def rows_kernel(
    depths, x_ref, out_ref, from_core, theirs, from_pair, to_send, from_depth, pieces, sems, more
):
    places = Places(depths)
    core, side = places.core, lax.axis_index("hidden")
    width = out_ref.shape[-1]
    greet(places, ("hidden", "rows"))
    halves = send(x_ref.at[:, 1 - core], from_core, sems, 2 * depths, places.to_core())
    halves.wait_recv()

    def part(which):
        columns = pl.ds(pl.multiple_of(which * width, 128), width)

        def at(depth):
            own = x_ref[depth, core, :, columns].astype(jnp.float32)
            return own + from_core[depth, :, columns].astype(jnp.float32)

        return at

    total = exchange_sum(
        places, "hidden", part(side), part(1 - side), theirs, from_pair, to_send, from_depth, sems
    )
    pieces[lax.axis_index("rows"), places.depth, core] = total.astype(pieces.dtype)
    halves.wait_send()
    spread(places, "rows", pieces, more)
    out_ref[...] = pieces[...]


def recon_kernel(
    depths,
    scale,
    x_ref,
    target_ref,
    bias_ref,
    err_ref,
    recon_ref,
    from_core,
    theirs,
    from_pair,
    to_send,
    from_depth,
    pieces,
    sems,
    more,
):
    places = Places(depths)
    core, side = places.core, lax.axis_index("rows")
    greet(places, ("rows",))
    halves = send(x_ref.at[:, :, 1 - core], from_core, sems, 2 * depths, places.to_core())
    halves.wait_recv()

    def part(which):
        def at(depth):
            own = x_ref[which, depth, core].astype(jnp.float32)
            return own + from_core[which, depth].astype(jnp.float32)

        return at

    total = exchange_sum(
        places, "rows", part(side), part(1 - side), theirs, from_pair, to_send, from_depth, sems
    )
    recon = total + bias_ref[...]
    recon_ref[...] = recon.astype(recon_ref.dtype)
    err = scale * (recon - target_ref[side, places.depth, core].astype(jnp.float32))
    pieces[side, places.depth, core] = err.astype(pieces.dtype)
    halves.wait_send()
    spread(places, "rows", pieces, more)
    err_ref[...] = pieces[...]


def vmem(count):
    return [pl.BlockSpec(memory_space=pltpu.VMEM)] * count


def params(number):
    return pltpu.CompilerParams(collective_id=number, has_side_effects=True)


def gather_features(x, depths):
    shape = (2, depths, 2) + x.shape
    out = pl.pallas_call(
        functools.partial(gather_kernel, "hidden", depths),
        out_shape=jax.ShapeDtypeStruct(shape, x.dtype),
        in_specs=vmem(1),
        out_specs=vmem(1)[0],
        scratch_shapes=[
            pltpu.VMEM(shape, x.dtype),
            pltpu.SemaphoreType.DMA((2, 4 * depths)),
        ],
        compiler_params=params(0),
        name="gather_features",
    )(x)
    return out.reshape(-1, x.shape[-1])


def reduce_scratch(depths, rows, width, core_shape, dtype):
    piece = (rows, width)
    return [
        pltpu.VMEM(core_shape, dtype),
        pltpu.VMEM((depths,) + piece, dtype),
        pltpu.VMEM((depths,) + piece, dtype),
        pltpu.VMEM((depths - 1,) + piece, dtype),
        pltpu.VMEM((depths - 1,) + piece, dtype),
        pltpu.VMEM((2, depths, 2) + piece, dtype),
        pltpu.SemaphoreType.DMA((2, 2 * depths + 1)),
        pltpu.SemaphoreType.DMA((2, 4 * depths)),
    ]


def sum_rows(x, depths):
    rows, width = x.shape[0] // (2 * depths), x.shape[1] // 2
    out = pl.pallas_call(
        functools.partial(rows_kernel, depths),
        out_shape=jax.ShapeDtypeStruct((2, depths, 2, rows, width), x.dtype),
        in_specs=vmem(1),
        out_specs=vmem(1)[0],
        scratch_shapes=reduce_scratch(
            depths, rows, width, (depths, rows, x.shape[1]), x.dtype
        ),
        compiler_params=params(1),
        name="sum_rows",
    )(x.reshape(depths, 2, rows, x.shape[1]))
    return out.reshape(-1, width)


def sum_recon(x, target, bias, scale, depths, number):
    tokens, width = x.shape
    rows = tokens // (4 * depths)
    shape = (2, depths, 2, rows, width)
    err, recon = pl.pallas_call(
        functools.partial(recon_kernel, depths, scale),
        out_shape=(
            jax.ShapeDtypeStruct(shape, x.dtype),
            jax.ShapeDtypeStruct((rows, width), x.dtype),
        ),
        in_specs=vmem(3),
        out_specs=tuple(vmem(2)),
        scratch_shapes=reduce_scratch(depths, rows, width, (2, depths, rows, width), x.dtype),
        compiler_params=params(number),
    )(x.reshape(shape), target.reshape(shape), bias[None, :])
    return err.reshape(tokens, width), recon


def turn_kernel(err_ref, decoder_ref, out_ref):
    out_ref[...] = lax.dot_general(
        err_ref[...],
        decoder_ref[...],
        (((1,), (1,)), ((), ())),
        preferred_element_type=jnp.float32,
    ).astype(out_ref.dtype)


def turn(err, decoder, which, count):
    size = decoder.shape[0] // count
    block = 512 if size % 512 == 0 else size
    steps = size // block
    return pl.pallas_call(
        turn_kernel,
        grid=(steps,),
        out_shape=jax.ShapeDtypeStruct((err.shape[0], size), err.dtype),
        in_specs=[
            pl.BlockSpec(err.shape, lambda i: (0, 0)),
            pl.BlockSpec((block, decoder.shape[1]), lambda i: (which * steps + i, 0)),
        ],
        out_specs=pl.BlockSpec((err.shape[0], block), lambda i: (0, i)),
        cost_estimate=pl.CostEstimate(
            flops=2 * err.size * size,
            bytes_accessed=2 * (err.size + size * decoder.shape[1] + err.shape[0] * size),
            transcendentals=0,
        ),
        name="turn",
    )(err, decoder)


def weight_kernel(count, left_ref, *refs):
    rights, out_ref, right = refs[:count], refs[-2], refs[-1]

    @pl.when(pl.program_id(0) == 0)
    def _():
        at = 0
        for ref in rights:
            right[at : at + ref.shape[0]] = ref[...]
            at += ref.shape[0]

    out_ref[...] = lax.dot_general(
        left_ref[...],
        right[...],
        (((0,), (0,)), ((), ())),
        preferred_element_type=jnp.float32,
    ).astype(out_ref.dtype)


def weight_columns(left, rights, which, count, into):
    tokens, features = left.shape
    size = rights[0].shape[1]
    block = 256 if features % 256 == 0 else features
    whole = pl.BlockSpec(rights[0].shape, lambda i: (0, 0))
    specs = [pl.BlockSpec((tokens, block), lambda i: (0, i))] + [whole] * len(rights)
    args = [left] + rights
    aliases = {}
    if into is not None:
        aliases = {len(args): 0}
        specs.append(pl.BlockSpec(memory_space=pl.ANY))
        args.append(into)
    return pl.pallas_call(
        functools.partial(weight_kernel, len(rights)),
        grid=(features // block,),
        out_shape=jax.ShapeDtypeStruct((features, size * count), left.dtype),
        in_specs=specs,
        out_specs=pl.BlockSpec((block, size), lambda i: (i, which)),
        scratch_shapes=[pltpu.VMEM((tokens, size), left.dtype)],
        input_output_aliases=aliases,
        cost_estimate=pl.CostEstimate(
            flops=2 * left.size * size,
            bytes_accessed=2 * (left.size + tokens * size + features * size),
            transcendentals=0,
        ),
    )(*args)


def after(x, *others):
    return lax.optimization_barrier((x,) + others)[0]


def add_pair(x, *others):
    if lax.axis_size("hidden") == 2:
        other = lax.ppermute(x, "hidden", [(0, 1), (1, 0)])
        other = after(other, *others) if others else other
        return x.astype(jnp.float32) + other.astype(jnp.float32)
    return lax.psum(x, "hidden").astype(jnp.float32)


def shards(
    inputs, gate_weight, up_weight, down_weight, encoder, decoder, enc_bias, dec_bias, shuffle_order
):
    rows_n, hidden_n, latents_n = map(lax.axis_size, ("rows", "hidden", "latents"))
    tokens = shuffle_order.shape[0]
    features = gate_weight.shape[0]
    depths = latents_n // 2
    fast = (
        rows_n == 2
        and hidden_n == 2
        and latents_n % 2 == 0
        and tokens % (2 * latents_n * 16) == 0
        and features % 256 == 0
        and inputs.shape[1] % 16 == 0
        and inputs.shape[0] % 128 == 0
    )
    if fast:
        gathered = gather_features(inputs.T, depths).T
    else:
        gathered = lax.all_gather(inputs, ("hidden", "latents"), axis=1, tiled=True)
    gate_act = jnp.dot(gathered, gate_weight, preferred_element_type=jnp.float32)
    up_act = jnp.dot(gathered, up_weight, preferred_element_type=jnp.float32)
    hidden = (jax.nn.gelu(gate_act, approximate=True) * up_act).astype(jnp.bfloat16)
    partial_value = jnp.dot(hidden, down_weight, preferred_element_type=jnp.float32)
    partial_value = partial_value.astype(jnp.bfloat16)
    if fast:
        every_row = sum_rows(partial_value, depths)
    else:
        share = lax.psum_scatter(partial_value, "hidden", scatter_dimension=1, tiled=True)
        width_rows = lax.psum(share, "latents")
        every_row = lax.all_gather(width_rows, "rows", axis=0, tiled=True)
    scale = 1.0 / math.sqrt(tokens)
    order = shuffle_order
    if fast:
        order = order.reshape(rows_n * latents_n, halves, -1).transpose(1, 0, 2).reshape(-1)
    columns = lax.broadcasted_iota(jnp.int32, (tokens, tokens), 1)
    one_hot = (order[:, None] == columns).astype(jnp.bfloat16)
    shuffled = jnp.dot(one_hot, every_row, preferred_element_type=jnp.float32)
    shuffled = shuffled.astype(jnp.bfloat16)

    count = chunks if encoder.shape[1] % (128 * chunks) == 0 else 1
    size = encoder.shape[1] // count
    cuts = [slice(i * size, (i + 1) * size) for i in range(count)]
    parts = halves if fast else 1
    share = tokens // parts
    rows = [shuffled[i * share : (i + 1) * share] for i in range(parts)]
    local = []
    for part in range(parts):
        if part:
            rows[part] = after(rows[part], *local[part - 1])
        local.append(
            [
                jnp.dot(
                    rows[part], encoder[:, cut], preferred_element_type=jnp.float32
                ).astype(jnp.bfloat16)
                for cut in cuts
            ]
        )
    pre_act, latent_act, recon_out, d_err, d_pre = [], [], [], [], []
    for part in range(parts):
        pre, latent = [], []
        recon_local = None
        for i, cut in enumerate(cuts):
            summed = add_pair(local[part][i], *d_err[part - 1 : part])
            pre.append(summed + enc_bias[None, cut])
            latent.append(
                (smooth_scale * jax.nn.softplus(pre[i] / smooth_scale)).astype(jnp.bfloat16)
            )
            term = jnp.dot(latent[i], decoder[cut], preferred_element_type=jnp.float32)
            recon_local = term if recon_local is None else recon_local + term
        pre_act.append(pre)
        latent_act.append(jnp.concatenate(latent, axis=1))
        if fast:
            err, recon_rows = sum_recon(
                recon_local.astype(jnp.bfloat16), rows[part], dec_bias, scale, depths, 2 + part
            )
        else:
            recon = lax.psum(recon_local, ("rows", "latents")) + dec_bias[None, :]
            err = (scale * (recon - rows[part].astype(jnp.float32))).astype(jnp.bfloat16)
            row_count = tokens // (rows_n * latents_n)
            first_row = lax.axis_index(("rows", "latents")) * row_count
            recon_rows = lax.dynamic_slice_in_dim(
                recon.astype(jnp.bfloat16), first_row, row_count, 0
            )
        recon_out.append(recon_rows)
        d_err.append(err)
    for part in range(parts):
        d_pre.append([])
        for i, cut in enumerate(cuts):
            if fast and turn_kernels:
                back_local = turn(d_err[part], decoder, i, count)
            else:
                back_local = lax.dot_general(
                    d_err[part],
                    decoder[cut],
                    (((1,), (1,)), ((), ())),
                    preferred_element_type=jnp.float32,
                ).astype(jnp.bfloat16)
            d_latent = add_pair(back_local)
            gate = jax.nn.sigmoid(pre_act[part][i] / smooth_scale)
            d_pre[part].append(
                ((d_latent + sparsity_weight * scale) * gate).astype(jnp.bfloat16)
            )
    grad_dec = lax.dot_general(
        jnp.concatenate(latent_act, axis=0),
        jnp.concatenate(d_err, axis=0),
        (((0,), (0,)), ((), ())),
        preferred_element_type=jnp.float32,
    ).astype(jnp.bfloat16)
    if fast:
        grad_enc = None
        for i in range(count):
            grad_enc = weight_columns(
                shuffled, [part[i] for part in d_pre], i, count, grad_enc
            )
    else:
        grad_enc = lax.dot_general(
            shuffled,
            jnp.concatenate([jnp.concatenate(part, axis=1) for part in d_pre], axis=0),
            (((0,), (0,)), ((), ())),
            preferred_element_type=jnp.float32,
        ).astype(jnp.bfloat16)
    return (jnp.concatenate(recon_out, axis=0), grad_enc, grad_dec)


def solution(mesh):
    return jax.shard_map(
        shards,
        mesh=mesh,
        in_specs=(
            P("rows", ("hidden", "latents")),
            P(None, ("hidden", "latents")),
            P(None, ("hidden", "latents")),
            P(("hidden", "latents"), None),
            P("hidden", ("rows", "latents")),
            P(("rows", "latents"), "hidden"),
            P(("rows", "latents")),
            P("hidden"),
            P(),
        ),
        out_specs=(
            P(("rows", "latents"), "hidden"),
            P("hidden", ("rows", "latents")),
            P(("rows", "latents"), "hidden"),
        ),
        check_vma=False,
    )
```
